32 devices in a mesh: rows: 8 (over z, y), slab: 4 (over x, core).
Axes of the slice: x: 2, y: 2, z: 4, core: 2. Of those that a mesh axis runs over, the one named last changes fastest.
Arguments:
- snapshots: bfloat16 [65536, 2048], P(('rows', 'slab')), may hold values from -60 to 60
- start_block: float32 [2048, 64], replicated, may hold values from -6 to 6
- linear_op: float32 [64, 64], replicated, may hold values from -0.75 to 0.75
- quad_op: float32 [4096, 64], replicated, may hold values from -0.009765625 to 0.009765625
- offset: float32 [64], replicated, may hold values from -3 to 3
Outputs:
- projection: bfloat16 [65536, 64], P(('rows', 'slab'))
- reduced: float32 [2048, 64], P(('rows', 'slab'))
- mismatch: float32 [2048, 64], P(('rows', 'slab'))
The draws below stay inside these ranges and needn't reach their ends.
All inputs are finite; a program needn't handle non-finite values.
Results may differ from the reference program's by a relative error of at most 0.0029.
Values sent between devices are 32-bit elements; how exact they have to be, the bound alone decides.
A program may use at most 128 MiB of HBM per device.

```python
import math
import jax
import jax.numpy as jnp
from jax import lax

K = 2048
RANK = 64
NROWS = 65536


def draw_snapshots(key, part):
    noise = jax.random.normal(key, (NROWS, K + 2), jnp.float32)
    mixed = noise[:, 2:] + 0.8 * noise[:, 1:-1] + 0.5 * noise[:, :-2]
    mixed = jnp.clip(mixed, -60.0, 60.0)
    return mixed.astype(jnp.bfloat16)


def bell_draw(rng, extent, scale, reach, kind=jnp.bfloat16):
    drawn = jax.random.normal(rng, extent, jnp.float32) * scale
    return jnp.minimum(jnp.maximum(drawn, -reach), reach).astype(kind)


def setup_inputs(seed: int = 0) -> dict:
    seeds = jax.random.split(jax.random.key(seed), 6)
    return {
        "snapshots": draw_snapshots(jax.random.fold_in(seeds[5], 71), 0),
        "start_block": bell_draw(seeds[1], (K, RANK), 1.0, 6.0, jnp.float32),
        "linear_op": bell_draw(seeds[2], (RANK, RANK), RANK ** -0.5, 0.75, jnp.float32),
        "quad_op": bell_draw(seeds[3], (RANK * RANK, RANK), (100 * RANK * RANK) ** -0.5, 0.009765625, jnp.float32),
        "offset": bell_draw(seeds[4], (RANK,), 0.5, 3.0, jnp.float32),
    }


def advance(state, linear_op, quad_op, offset):
    pairs = (state[:, :, None] * state[:, None, :]).reshape(state.shape[0], -1)
    hp = lax.Precision.HIGHEST
    change = jnp.dot(state, linear_op, precision=hp) + jnp.dot(pairs, quad_op, precision=hp) + offset[None, :]
    return state + 0.25 * change

def reference(snapshots, start_block, linear_op, quad_op, offset):
    hp = lax.Precision.HIGHEST
    total = snapshots.shape[0]
    width = snapshots.shape[1]
    block = math.gcd(total, 8192)
    pieces = snapshots.reshape(total // block, block, width)

    def power_step(acc, piece):
        floats = piece.astype(jnp.float32)
        inner = jnp.dot(floats, start_block, precision=hp)
        return (acc + jnp.dot(floats.T, inner, precision=hp), None)
    power, _ = lax.scan(power_step, jnp.zeros((width, RANK), jnp.float32), pieces)
    correlation = jnp.dot(power.T, power, precision=hp)
    factor = jnp.linalg.cholesky(correlation)
    basis = jax.scipy.linalg.solve_triangular(factor, power.T, lower=True).T

    def coord_step(acc, piece):
        floats = piece.astype(jnp.float32)
        modes = jnp.dot(floats, basis, precision=hp)
        return (acc + jnp.dot(floats.T, modes, precision=hp), modes.astype(jnp.bfloat16))
    coords, modes = lax.scan(coord_step, jnp.zeros((width, RANK), jnp.float32), pieces)
    projection = modes.reshape(total, RANK)
    reduced = coords * (math.sqrt(width) / total)
    state = advance(advance(reduced, linear_op, quad_op, offset), linear_op, quad_op, offset)
    target = jnp.concatenate([reduced[2:], jnp.zeros((2, RANK), jnp.float32)], axis=0)
    index = jnp.arange(width, dtype=jnp.int32)
    mismatch = jnp.where((index < width - 2)[:, None], state - target, jnp.float32(0.0))
    return (projection, reduced, mismatch)
```

```python
import functools
import math

import jax
import jax.numpy as jnp
from jax import lax
from jax.experimental import pallas as pl
from jax.experimental.pallas import tpu as pltpu
from jax.sharding import PartitionSpec as P

MESH = pl.DeviceIdType.MESH
LANES = 128
SUBLANES = 8
VMEM_SPEC = pl.BlockSpec(memory_space=pltpu.VMEM)
F32 = jnp.float32
BF16 = jnp.bfloat16
HIGHEST = lax.Precision.HIGHEST


def split(x):
    high = x.astype(BF16)
    low = (x - high.astype(F32)).astype(BF16)
    return high, low


def dot(a, b, contract):
    return lax.dot_general(a, b, (contract, ((), ())), preferred_element_type=F32)


def pass_over(snap_ref, cat_ref, acc_ref):
    rank = cat_ref.shape[1] // 2
    step = pl.program_id(0)
    both = dot(snap_ref[...], cat_ref[...], ((1,), (0,)))
    y = both[:, :rank] + both[:, rank:]
    high, low = split(y)
    ycat = jnp.concatenate([high, low], axis=1)
    part = dot(ycat, snap_ref[...], ((0,), (0,)))
    folded = part[:rank] + part[rank:]

    @pl.when(step == 0)
    def _():
        acc_ref[...] = folded

    @pl.when(step > 0)
    def _():
        acc_ref[...] += folded

    return y


def power_kernel(snap_ref, start_ref, out_ref, cat_ref, acc_ref):
    @pl.when(pl.program_id(0) == 0)
    def _():
        cat_ref[...] = jnp.concatenate(split(start_ref[...]), axis=1)

    pass_over(snap_ref, cat_ref, acc_ref)

    @pl.when(pl.program_id(0) == pl.num_programs(0) - 1)
    def _():
        rank, width = acc_ref.shape
        per_row = width // LANES
        per_chunk = out_ref.shape[1] // SUBLANES
        for t in range(rank // SUBLANES * per_row):
            i, j = divmod(t, per_row)
            tile = acc_ref[i * SUBLANES : (i + 1) * SUBLANES, j * LANES : (j + 1) * LANES]
            d, r = divmod(t, per_chunk)
            out_ref[d, r * SUBLANES : (r + 1) * SUBLANES, :] = tile


def coords_kernel(snap_ref, power_ref, out_ref, w_ref, corr_ref, cat_ref, acc_ref):
    @pl.when(pl.program_id(0) == 0)
    def _():
        pt = power_ref[...]
        cat_ref[...] = jnp.concatenate(split(pt.T), axis=1)
        high, low = split(pt)
        contract = ((1,), (1,))
        corr_ref[...] = dot(high, high, contract) + (dot(high, low, contract) + dot(low, high, contract))

    w_ref[...] = pass_over(snap_ref, cat_ref, acc_ref)

    @pl.when(pl.program_id(0) == pl.num_programs(0) - 1)
    def _():
        n, rows, _ = out_ref.shape
        share = acc_ref.shape[1] // n
        groups = LANES // share
        for d in range(n):
            lo = d * share
            parts = [acc_ref[g * rows : (g + 1) * rows, lo : lo + share] for g in range(groups)]
            out_ref[d] = jnp.concatenate(parts, axis=1) if groups > 1 else parts[0]


def place(index, slab):
    return (index // slab, lax.rem(index, slab))


def everyone(n, slab, me, fn):
    def one(s, _):
        peer = lax.rem(me + s, n)
        fn(s, peer, place(peer, slab))
        return 0

    lax.fori_loop(1, n, one, 0)


def enter(n, slab, me):
    barrier = pltpu.get_barrier_semaphore()
    everyone(
        n, slab, me,
        lambda s, peer, where: pl.semaphore_signal(barrier, inc=1, device_id=where, device_id_type=MESH),
    )
    pl.semaphore_wait(barrier, n - 1)


def scatter_copy(part_ref, recv_ref, send_sem, recv_sem, s, peer, where):
    return pltpu.make_async_remote_copy(
        src_ref=part_ref.at[peer], dst_ref=recv_ref.at[s],
        send_sem=send_sem.at[s], recv_sem=recv_sem.at[s],
        device_id=where, device_id_type=MESH,
    )


def total_of(n, me, part_ref, recv_ref):
    total = part_ref[me]
    return lax.fori_loop(1, n, lambda s, t: t + recv_ref[s], total)


def reduce_kernel(n, slab, part_ref, out_ref, recv_ref, full_ref, send_sem, recv_sem, send2, recv2):
    me = lax.axis_index(("rows", "slab"))
    enter(n, slab, me)
    make = functools.partial(scatter_copy, part_ref, recv_ref, send_sem, recv_sem)
    everyone(n, slab, me, lambda *a: make(*a).start())
    everyone(n, slab, me, lambda *a: make(*a).wait_recv())
    full_ref[me] = total_of(n, me, part_ref, recv_ref)

    def spread(s, peer, where):
        return pltpu.make_async_remote_copy(
            src_ref=full_ref.at[me], dst_ref=full_ref.at[me],
            send_sem=send2.at[s], recv_sem=recv2.at[s],
            device_id=where, device_id_type=MESH,
        )

    def arrival(s, peer, where):
        source = lax.rem(me + n - s, n)
        return pltpu.make_async_remote_copy(
            src_ref=full_ref.at[source], dst_ref=full_ref.at[source],
            send_sem=send2.at[s], recv_sem=recv2.at[s],
            device_id=where, device_id_type=MESH,
        )

    everyone(n, slab, me, lambda *a: spread(*a).start())
    everyone(n, slab, me, lambda *a: arrival(*a).wait_recv())
    rank, width = out_ref.shape
    per_row = width // LANES
    per_chunk = full_ref.shape[1] // SUBLANES
    for t in range(rank // SUBLANES * per_row):
        i, j = divmod(t, per_row)
        d, r = divmod(t, per_chunk)
        tile = full_ref[d, r * SUBLANES : (r + 1) * SUBLANES, :]
        out_ref[i * SUBLANES : (i + 1) * SUBLANES, j * LANES : (j + 1) * LANES] = tile
    everyone(n, slab, me, lambda *a: make(*a).wait_send())
    everyone(n, slab, me, lambda *a: spread(*a).wait_send())


def invert_factor(corr, work_ref):
    rank = corr.shape[0]
    row = lax.broadcasted_iota(jnp.int32, (rank, rank), 0)
    col = lax.broadcasted_iota(jnp.int32, (rank, rank), 1)
    eye = jnp.where(row == col, 1.0, 0.0).astype(F32)
    work_ref[...] = jnp.concatenate([corr, eye], axis=1)
    rows1 = lax.broadcasted_iota(jnp.int32, (rank, 1), 0)
    lanes = lax.broadcasted_iota(jnp.int32, (rank, 2 * rank), 1)
    lane1 = lax.broadcasted_iota(jnp.int32, (1, 2 * rank), 1)

    def eliminate(j, _):
        m = work_ref[...]
        pivot = work_ref[pl.ds(j, 1), :]
        column = jnp.sum(jnp.where(lanes == j, m, 0.0), axis=1, keepdims=True)
        d = jnp.sum(jnp.where(lane1 == j, pivot, 0.0), axis=1, keepdims=True)
        factor = jnp.where(rows1 > j, column / d, 0.0)
        work_ref[...] = m - factor * pivot
        return 0

    lax.fori_loop(0, rank, eliminate, 0)
    m = work_ref[...]
    diag = jnp.sum(jnp.where(row == col, m[:, :rank], 0.0), axis=1, keepdims=True)
    return m[:, rank:] / jnp.sqrt(diag)


def finish_kernel(n, slab, scale, part_ref, corr_ref, w_ref, lin_ref, quad_ref, off_ref,
                  proj_ref, red_ref, mis_ref,
                  recv_ref, work_ref, qcat_ref, edge_ref, halo_ref, send_sem, recv_sem, edge_send, edge_recv):
    me = lax.axis_index(("rows", "slab"))
    enter(n, slab, me)
    make = functools.partial(scatter_copy, part_ref, recv_ref, send_sem, recv_sem)
    everyone(n, slab, me, lambda *a: make(*a).start())

    inverse = invert_factor(corr_ref[...], work_ref)
    ihigh, ilow = split(inverse)
    nt = ((1,), (1,))
    block = min(w_ref.shape[0], 512)

    def modes_of(b, _):
        rows = pl.ds(pl.multiple_of(b * block, block), block)
        whigh, wlow = split(w_ref[rows, :])
        modes = dot(whigh, ihigh, nt) + (dot(whigh, ilow, nt) + dot(wlow, ihigh, nt))
        proj_ref[rows, :] = modes.astype(BF16)
        return 0

    lax.fori_loop(0, w_ref.shape[0] // block, modes_of, 0)
    rank = inverse.shape[0]
    qt = quad_ref[...].T
    qhigh, qlow = split(qt)
    qcat_ref[:rank, :] = qhigh
    qcat_ref[rank:, :] = qlow
    lin_t = lin_ref[...].T
    off_t = off_ref[...].T

    everyone(n, slab, me, lambda *a: make(*a).wait_recv())
    total = total_of(n, me, part_ref, recv_ref)
    share = red_ref.shape[0]
    groups = LANES // share
    if groups > 1:
        total = jnp.concatenate([total[:, g * share : (g + 1) * share] for g in range(groups)], axis=0)
    z = jnp.dot(inverse, total, precision=HIGHEST, preferred_element_type=F32) * scale
    reduced = z.T
    red_ref[...] = reduced
    edge_ref[...] = reduced[:SUBLANES]

    before = place(lax.rem(me + n - 1, n), slab)
    edge = pltpu.make_async_remote_copy(
        src_ref=edge_ref, dst_ref=halo_ref, send_sem=edge_send, recv_sem=edge_recv,
        device_id=before, device_id_type=MESH,
    )
    edge.start()

    state = z
    for _ in range(2):
        pairs = (state[:, None, :] * state[None, :, :]).reshape(rank * rank, share)
        phigh, plow = split(pairs)
        nn = ((1,), (0,))
        both = dot(qcat_ref[...], phigh, nn)
        quad = both[:rank] + (both[rank:] + dot(qcat_ref[:rank, :], plow, nn))
        change = jnp.dot(lin_t, state, precision=HIGHEST, preferred_element_type=F32) + quad + off_t
        state = state + 0.25 * change
    rolled = state.T
    edge.wait_recv()
    target = jnp.concatenate([reduced[2:], halo_ref[...][:2]], axis=0)
    position = me * share + lax.broadcasted_iota(jnp.int32, (share, 1), 0)
    mis_ref[...] = jnp.where(position < n * share - 2, rolled - target, 0.0)
    edge.wait_send()
    everyone(n, slab, me, lambda *a: make(*a).wait_send())


def body(snapshots, start_block, linear_op, quad_op, offset, *, n, slab):
    rows, width = snapshots.shape
    rank = start_block.shape[1]
    share = width // n
    tiles = rank * width // n // LANES
    scale = math.sqrt(width) / (rows * n)
    block = min(rows, 512)
    snap_spec = pl.BlockSpec((block, width), lambda i: (i, 0))
    whole = lambda shape: pl.BlockSpec(shape, lambda i: (0,) * len(shape))
    scratch = [pltpu.VMEM((width, 2 * rank), BF16), pltpu.VMEM((rank, width), F32)]
    arbitrary = pltpu.CompilerParams(dimension_semantics=("arbitrary",), vmem_limit_bytes=56 * 2**20)
    cost = pl.CostEstimate(flops=8 * rows * width * rank, bytes_accessed=rows * width * 2, transcendentals=0)
    part = pl.pallas_call(
        power_kernel,
        grid=(rows // block,),
        in_specs=[snap_spec, whole((width, rank))],
        out_specs=whole((n, tiles, LANES)),
        out_shape=jax.ShapeDtypeStruct((n, tiles, LANES), F32),
        scratch_shapes=scratch, compiler_params=arbitrary, cost_estimate=cost, name="power",
    )(snapshots, start_block)

    sems = lambda: pltpu.SemaphoreType.DMA((n,))
    power_t = pl.pallas_call(
        functools.partial(reduce_kernel, n, slab),
        in_specs=[VMEM_SPEC],
        out_specs=VMEM_SPEC,
        out_shape=jax.ShapeDtypeStruct((rank, width), F32),
        scratch_shapes=[pltpu.VMEM((n, tiles, LANES), F32), pltpu.VMEM((n, tiles, LANES), F32), sems(), sems(), sems(), sems()],
        compiler_params=pltpu.CompilerParams(collective_id=0, has_side_effects=True),
        name="allreduce",
    )(part)

    zpart, w, corr = pl.pallas_call(
        coords_kernel,
        grid=(rows // block,),
        in_specs=[snap_spec, whole((rank, width))],
        out_specs=[whole((n, tiles, LANES)), pl.BlockSpec((block, rank), lambda i: (i, 0)), whole((rank, rank))],
        out_shape=[
            jax.ShapeDtypeStruct((n, tiles, LANES), F32),
            jax.ShapeDtypeStruct((rows, rank), F32),
            jax.ShapeDtypeStruct((rank, rank), F32),
        ],
        scratch_shapes=scratch, compiler_params=arbitrary, cost_estimate=cost, name="coords",
    )(snapshots, power_t)

    return pl.pallas_call(
        functools.partial(finish_kernel, n, slab, scale),
        in_specs=[VMEM_SPEC] * 6,
        out_specs=[VMEM_SPEC] * 3,
        out_shape=[
            jax.ShapeDtypeStruct((rows, rank), BF16),
            jax.ShapeDtypeStruct((share, rank), F32),
            jax.ShapeDtypeStruct((share, rank), F32),
        ],
        scratch_shapes=[
            pltpu.VMEM((n, tiles, LANES), F32),
            pltpu.VMEM((rank, 2 * rank), F32),
            pltpu.VMEM((2 * rank, rank * rank), BF16),
            pltpu.VMEM((SUBLANES, rank), F32),
            pltpu.VMEM((SUBLANES, rank), F32),
            sems(), sems(), pltpu.SemaphoreType.DMA, pltpu.SemaphoreType.DMA,
        ],
        compiler_params=pltpu.CompilerParams(collective_id=1, has_side_effects=True, vmem_limit_bytes=56 * 2**20),
        name="finish",
    )(zpart, corr, w, linear_op, quad_op, offset.reshape(1, rank))


def solution(mesh):
    in_specs = (P(("rows", "slab"), None), P(), P(), P(), P())
    out_specs = (P(("rows", "slab"), None), P(("rows", "slab"), None), P(("rows", "slab"), None))
    slab = mesh.shape["slab"]
    run = functools.partial(body, n=mesh.shape["rows"] * slab, slab=slab)
    return jax.shard_map(run, mesh=mesh, in_specs=in_specs, out_specs=out_specs, check_vma=False)
```

```python
import functools
import math

import jax
import jax.numpy as jnp
from jax import lax
from jax.experimental import pallas as pl
from jax.experimental.pallas import tpu as pltpu
from jax.sharding import PartitionSpec as P

MESH = pl.DeviceIdType.MESH
LANES = 128
SUBLANES = 8
BLOCK = 2 * LANES
LAG = 2
VMEM_SPEC = pl.BlockSpec(memory_space=pltpu.VMEM)
ANY_SPEC = pl.BlockSpec(memory_space=pl.ANY)
F32 = jnp.float32
BF16 = jnp.bfloat16
HIGHEST = lax.Precision.HIGHEST
NN = ((1,), (0,))
NT = ((1,), (1,))


def split(x):
    high = x.astype(BF16)
    low = (x - high.astype(F32)).astype(BF16)
    return high, low


def dot(a, b, contract=NN):
    return lax.dot_general(a, b, (contract, ((), ())), preferred_element_type=F32)


class Layout:
    def __init__(self, rows, slab, core_axis):
        self.rows, self.slab, self.core_axis = rows, slab, core_axis
        self.n = rows * slab
        self.m = self.n // 2

    def split_index(self, r, s):
        if self.core_axis == "slab":
            return r * (self.slab // 2) + s // 2, s % 2
        return (r // 2) * self.slab + s, r % 2

    def place(self, q, c):
        if self.core_axis == "slab":
            half = self.slab // 2
            return q // half, 2 * (q % half) + c
        return 2 * (q // self.slab) + c, q % self.slab

    def of_device(self, d):
        return self.split_index(d // self.slab, d % self.slab)


def remote(src, dst, send, recv, where):
    return pltpu.make_async_remote_copy(
        src_ref=src, dst_ref=dst, send_sem=send, recv_sem=recv, device_id=where, device_id_type=MESH
    )


def pack(folded, share):
    groups = LANES // share
    rows = folded.shape[0] // groups
    if groups == 1:
        return folded
    return jnp.concatenate([folded[g * rows : (g + 1) * rows] for g in range(groups)], axis=1)


def unpack(chunk, share):
    groups = LANES // share
    if groups == 1:
        return chunk
    return jnp.concatenate([chunk[:, g * share : (g + 1) * share] for g in range(groups)], axis=0)


def kernel(lay, scale, snap_ref, start_ref, lin_ref, quad_ref, off_ref,
           proj_ref, red_ref, mis_ref,
           s_ref, cat_ref, yt_ref, pt_ref, quad_vmem, qcat_ref, work_ref, edge_ref, halo_ref, full_ref,
           part1, got1, mine1, recv1, part2, got2, mine2, recv2,
           load_sem, quad_sem, pair_send1, pair_recv1, far_send1, far_recv1,
           pair_send2, pair_recv2, far_send2, far_recv2,
           all_send, all_recv, fwd_send, fwd_recv, edge_send, edge_recv):
    n, m = lay.n, lay.m
    r, s = lax.axis_index("rows"), lax.axis_index("slab")
    me = r * lay.slab + s
    q, c = lay.split_index(r, s)
    partner = lay.place(q, 1 - c)
    rows, width = s_ref.shape
    rank = pt_ref.shape[0]
    share = width // n
    blocks = width // BLOCK
    qpb = m // blocks
    load = load_sem.shape[0]
    chunk = rows // load

    def fetch(b):
        at = pl.ds(b * chunk, chunk)
        return pltpu.make_async_copy(snap_ref.at[at], s_ref.at[at], load_sem.at[b])

    for b in range(load):
        fetch(b).start()
    quad_copy = pltpu.make_async_copy(quad_ref, quad_vmem, quad_sem)
    quad_copy.start()

    barrier = pltpu.get_barrier_semaphore()

    def greet(i, _):
        peer = (me + i) % n
        pl.semaphore_signal(barrier, inc=1, device_id=(peer // lay.slab, peer % lay.slab), device_id_type=MESH)
        return 0

    lax.fori_loop(1, n, greet, 0)

    def forward(b):
        both = dot(s_ref[b * chunk : (b + 1) * chunk, :], cat_ref[...])
        y = (both[:, :rank] + both[:, rank:]).T
        high, low = split(y)
        yt_ref[:rank, b * chunk : (b + 1) * chunk] = high
        yt_ref[rank:, b * chunk : (b + 1) * chunk] = low

    def each_other(fn):
        def one(i, _):
            fn((q + i) % m)
            return 0

        lax.fori_loop(1, m, one, 0)

    def scatter(part, got, mine, recv, pair_send, pair_recv, far_send, far_recv):
        def pair_copy(k):
            at = pl.ds(k * qpb, qpb)
            return remote(part.at[1 - c, at], got.at[at], pair_send.at[k], pair_recv.at[k], partner)

        def far_copy(target):
            return remote(mine.at[target], recv.at[q], far_send.at[target], far_recv.at[q], lay.place(target, c))

        def arrival(source):
            return remote(mine.at[source], recv.at[source], far_send.at[source], far_recv.at[source], lay.place(source, c))

        def relay(k):
            pair_copy(k).wait_recv()
            at = pl.ds(k * qpb, qpb)
            mine[at] = part[c, at] + got[at]
            for i in range(qpb):
                target = k * qpb + i

                @pl.when(target != q)
                def _():
                    far_copy(target).start()

        for k in range(blocks):
            both = dot(yt_ref[...], s_ref[:, k * BLOCK : (k + 1) * BLOCK])
            folded = both[:rank] + both[rank:]
            for i in range(BLOCK // share):
                dq, dc = lay.of_device(k * (BLOCK // share) + i)
                part[dc, dq] = pack(folded[:, i * share : (i + 1) * share], share)
            if k == 0 and part is part1:
                pl.semaphore_wait(barrier, n - 1)
            pair_copy(k).start()
            if k >= LAG:
                relay(k - LAG)
        for k in range(blocks - LAG, blocks):
            relay(k)

        def collect():
            def one(i, total):
                source = (q + i) % m
                arrival(source).wait_recv()
                return total + recv[source]

            return lax.fori_loop(1, m, one, mine[q])

        def drain():
            for k in range(blocks):
                pair_copy(k).wait_send()
            each_other(lambda target: far_copy(target).wait_send())

        return collect, drain

    cat_ref[...] = jnp.concatenate(split(start_ref[...].T), axis=1)
    for b in range(load):
        fetch(b).wait()
        forward(b)
    collect1, drain1 = scatter(part1, got1, mine1, recv1, pair_send1, pair_recv1, far_send1, far_recv1)
    full_ref[c, q] = collect1()

    def spread(target):
        return remote(full_ref.at[c, q], full_ref.at[c, q], all_send.at[target], all_recv.at[q], lay.place(target, c))

    def landed(source):
        return remote(
            full_ref.at[c, source], full_ref.at[c, source], all_send.at[source], all_recv.at[source], lay.place(source, c)
        )

    def across(source, half):
        return remote(
            full_ref.at[half, source], full_ref.at[half, source], fwd_send.at[source], fwd_recv.at[source], partner
        )

    each_other(lambda target: spread(target).start())
    across(q, c).start()

    def pass_on(source):
        landed(source).wait_recv()
        across(source, c).start()

    each_other(pass_on)
    across(q, 1 - c).wait_recv()
    each_other(lambda source: across(source, 1 - c).wait_recv())

    per = LANES // share
    for b in range(width // LANES):
        pieces = []
        for i in range(per):
            dq, dc = lay.of_device(b * per + i)
            pieces.append(unpack(full_ref[dc, dq], share))
        pt_ref[:, b * LANES : (b + 1) * LANES] = jnp.concatenate(pieces, axis=1) if per > 1 else pieces[0]
    cat_ref[...] = jnp.concatenate(split(pt_ref[...].T), axis=1)
    for b in range(load):
        forward(b)
    collect2, drain2 = scatter(part2, got2, mine2, recv2, pair_send2, pair_recv2, far_send2, far_recv2)

    phigh, plow = split(pt_ref[...])
    corr = dot(phigh, phigh, NT) + (dot(phigh, plow, NT) + dot(plow, phigh, NT))
    inverse = invert_factor(corr, work_ref)
    icat = jnp.concatenate(split(inverse), axis=0)
    ihigh = icat[:rank]
    for b in range(load):
        at = slice(b * chunk, (b + 1) * chunk)
        both = dot(icat, yt_ref[:rank, at])
        modes = both[:rank] + (both[rank:] + dot(ihigh, yt_ref[rank:, at]))
        proj_ref[:, at] = modes.astype(BF16)
    quad_copy.wait()
    qhigh, qlow = split(quad_vmem[...])
    qcat_ref[:rank, :] = qhigh
    qcat_ref[rank:, :] = qlow

    z = jnp.dot(inverse, unpack(collect2(), share), precision=HIGHEST, preferred_element_type=F32) * scale
    red_ref[...] = z
    edge_ref[...] = z.T[:SUBLANES]
    before = (me + n - 1) % n
    edge = remote(edge_ref, halo_ref, edge_send, edge_recv, (before // lay.slab, before % lay.slab))
    edge.start()

    state = z
    for _ in range(2):
        pairs = (state[:, None, :] * state[None, :, :]).reshape(rank * rank, share)
        pair_high, pair_low = split(pairs)
        both = dot(qcat_ref[...], pair_high)
        quad = both[:rank] + (both[rank:] + dot(qcat_ref[:rank, :], pair_low))
        change = jnp.dot(lin_ref[...], state, precision=HIGHEST, preferred_element_type=F32) + quad + off_ref[...]
        state = state + 0.25 * change
    edge.wait_recv()
    target = jnp.concatenate([z[:, 2:], halo_ref[...].T[:, :2]], axis=1)
    position = me * share + lax.broadcasted_iota(jnp.int32, (1, share), 1)
    mis_ref[...] = jnp.where(position < width - 2, state - target, 0.0)

    edge.wait_send()
    drain1()
    drain2()
    each_other(lambda other: spread(other).wait_send())
    across(q, c).wait_send()
    each_other(lambda other: across(other, c).wait_send())


def invert_factor(corr, work_ref):
    rank = corr.shape[0]
    row = lax.broadcasted_iota(jnp.int32, (rank, rank), 0)
    col = lax.broadcasted_iota(jnp.int32, (rank, rank), 1)
    eye = jnp.where(row == col, 1.0, 0.0).astype(F32)
    work_ref[...] = jnp.concatenate([corr, eye], axis=1)
    rows1 = lax.broadcasted_iota(jnp.int32, (rank, 1), 0)
    lanes = lax.broadcasted_iota(jnp.int32, (rank, 2 * rank), 1)
    lane1 = lax.broadcasted_iota(jnp.int32, (1, 2 * rank), 1)

    def eliminate(j, _):
        m = work_ref[...]
        pivot = work_ref[pl.ds(j, 1), :]
        column = jnp.sum(jnp.where(lanes == j, m, 0.0), axis=1, keepdims=True)
        d = jnp.sum(jnp.where(lane1 == j, pivot, 0.0), axis=1, keepdims=True)
        factor = jnp.where(rows1 > j, column / d, 0.0)
        work_ref[...] = m - factor * pivot
        return 0

    lax.fori_loop(0, rank, eliminate, 0)
    m = work_ref[...]
    diag = jnp.sum(jnp.where(row == col, m[:, :rank], 0.0), axis=1, keepdims=True)
    return m[:, rank:] / jnp.sqrt(diag)


def body(snapshots, start_block, linear_op, quad_op, offset, *, lay):
    rows, width = snapshots.shape
    rank = start_block.shape[1]
    n, m = lay.n, lay.m
    share = width // n
    tall = rank * share // LANES
    blocks = width // BLOCK
    load = 4
    scale = math.sqrt(width) / (rows * n)
    dma = lambda k: pltpu.SemaphoreType.DMA((k,))
    half = lambda: pltpu.VMEM((m, tall, LANES), F32)
    both = lambda: pltpu.VMEM((2, m, tall, LANES), F32)
    one = pltpu.SemaphoreType.DMA
    projection, reduced, mismatch = pl.pallas_call(
        functools.partial(kernel, lay, scale),
        in_specs=[ANY_SPEC, VMEM_SPEC, VMEM_SPEC, ANY_SPEC, VMEM_SPEC],
        out_specs=[VMEM_SPEC] * 3,
        out_shape=[
            jax.ShapeDtypeStruct((rank, rows), BF16),
            jax.ShapeDtypeStruct((rank, share), F32),
            jax.ShapeDtypeStruct((rank, share), F32),
        ],
        scratch_shapes=[
            pltpu.VMEM((rows, width), BF16),
            pltpu.VMEM((width, 2 * rank), BF16),
            pltpu.VMEM((2 * rank, rows), BF16),
            pltpu.VMEM((rank, width), F32),
            pltpu.VMEM((rank, rank * rank), F32),
            pltpu.VMEM((2 * rank, rank * rank), BF16),
            pltpu.VMEM((rank, 2 * rank), F32),
            pltpu.VMEM((SUBLANES, rank), F32),
            pltpu.VMEM((SUBLANES, rank), F32),
            both(),
            both(), half(), half(), half(),
            both(), half(), half(), half(),
            dma(load), one,
            dma(blocks), dma(blocks), dma(m), dma(m),
            dma(blocks), dma(blocks), dma(m), dma(m),
            dma(m), dma(m), dma(m), dma(m), one, one,
        ],
        compiler_params=pltpu.CompilerParams(collective_id=0, has_side_effects=True, vmem_limit_bytes=58 * 2**20),
        name="inference",
    )(snapshots, start_block.T, linear_op.T, quad_op.T, offset.reshape(rank, 1))
    return projection.T, reduced.T, mismatch.T


def solution(mesh):
    in_specs = (P(("rows", "slab"), None), P(), P(), P(), P())
    out_specs = (P(("rows", "slab"), None), P(("rows", "slab"), None), P(("rows", "slab"), None))
    grid = mesh.devices
    chip = lambda device: getattr(device, "coords", None)
    rows, slab = mesh.shape["rows"], mesh.shape["slab"]
    paired_rows = rows > 1 and chip(grid[0, 0]) is not None and chip(grid[0, 0]) == chip(grid[1, 0])
    lay = Layout(rows, slab, "rows" if paired_rows or slab % 2 else "slab")
    run = functools.partial(body, lay=lay)
    return jax.shard_map(run, mesh=mesh, in_specs=in_specs, out_specs=out_specs, check_vma=False)
```

```python
import functools
import math

import jax
import jax.numpy as jnp
from jax import lax
from jax.experimental import pallas as pl
from jax.experimental.pallas import tpu as pltpu
from jax.sharding import PartitionSpec as P

MESH = pl.DeviceIdType.MESH
LANES = 128
SUBLANES = 8
BLOCK = 2 * LANES
LAG = 2
VMEM_SPEC = pl.BlockSpec(memory_space=pltpu.VMEM)
ANY_SPEC = pl.BlockSpec(memory_space=pl.ANY)
F32 = jnp.float32
BF16 = jnp.bfloat16
HIGHEST = lax.Precision.HIGHEST
NN = ((1,), (0,))
NT = ((1,), (1,))


def split(x):
    high = x.astype(BF16)
    low = (x - high.astype(F32)).astype(BF16)
    return high, low


def dot(a, b, contract=NN):
    return lax.dot_general(a, b, (contract, ((), ())), preferred_element_type=F32)


class Layout:
    def __init__(self, rows, slab, core_axis):
        self.rows, self.slab, self.core_axis = rows, slab, core_axis
        self.n = rows * slab
        self.m = self.n // 2

    def split_index(self, r, s):
        if self.core_axis == "slab":
            return r * (self.slab // 2) + s // 2, s % 2
        return (r // 2) * self.slab + s, r % 2

    def place(self, q, c):
        if self.core_axis == "slab":
            half = self.slab // 2
            return q // half, 2 * (q % half) + c
        return 2 * (q // self.slab) + c, q % self.slab

    def of_device(self, d):
        return self.split_index(d // self.slab, d % self.slab)


def remote(src, dst, send, recv, where):
    return pltpu.make_async_remote_copy(
        src_ref=src, dst_ref=dst, send_sem=send, recv_sem=recv, device_id=where, device_id_type=MESH
    )


def pack(folded, share):
    groups = LANES // share
    rows = folded.shape[0] // groups
    if groups == 1:
        return folded
    return jnp.concatenate([folded[g * rows : (g + 1) * rows] for g in range(groups)], axis=1)


def unpack(chunk, share):
    groups = LANES // share
    if groups == 1:
        return chunk
    return jnp.concatenate([chunk[:, g * share : (g + 1) * share] for g in range(groups)], axis=0)


def kernel(lay, scale, snap_ref, start_ref, lin_ref, quad_ref, off_ref,
           proj_ref, red_ref, mis_ref,
           s_ref, cat_ref, yt_ref, pt_ref, quad_vmem, qcat_ref, work_ref, edge_ref, halo_ref, full_ref,
           part1, got1, mine1, recv1, part2, got2, mine2, recv2,
           load_sem, quad_sem, pair_send1, pair_recv1, far_send1, far_recv1,
           pair_send2, pair_recv2, far_send2, far_recv2,
           all_send, all_recv, fwd_send, fwd_recv, edge_send, edge_recv):
    n, m = lay.n, lay.m
    r, s = lax.axis_index("rows"), lax.axis_index("slab")
    me = r * lay.slab + s
    q, c = lay.split_index(r, s)
    partner = lay.place(q, 1 - c)
    rows, width = s_ref.shape
    rank = pt_ref.shape[0]
    share = width // n
    blocks = width // BLOCK
    qpb = m // blocks
    load = load_sem.shape[0]
    chunk = rows // load

    def fetch(b):
        at = pl.ds(b * chunk, chunk)
        return pltpu.make_async_copy(snap_ref.at[at], s_ref.at[at], load_sem.at[b])

    for b in range(load):
        fetch(b).start()
    quad_copy = pltpu.make_async_copy(quad_ref, quad_vmem, quad_sem)
    quad_copy.start()

    barrier = pltpu.get_barrier_semaphore()

    def greet(i, _):
        peer = (me + i) % n
        pl.semaphore_signal(barrier, inc=1, device_id=(peer // lay.slab, peer % lay.slab), device_id_type=MESH)
        return 0

    lax.fori_loop(1, n, greet, 0)

    def forward(b):
        both = dot(s_ref[b * chunk : (b + 1) * chunk, :], cat_ref[...])
        y = (both[:, :rank] + both[:, rank:]).T
        high, low = split(y)
        yt_ref[:rank, b * chunk : (b + 1) * chunk] = high
        yt_ref[rank:, b * chunk : (b + 1) * chunk] = low

    def each_other(fn):
        def one(i, _):
            fn((q + i) % m)
            return 0

        lax.fori_loop(1, m, one, 0)

    def scatter(part, got, mine, recv, pair_send, pair_recv, far_send, far_recv):
        def pair_copy(k):
            at = pl.ds(k * qpb, qpb)
            return remote(part.at[1 - c, at], got.at[at], pair_send.at[k], pair_recv.at[k], partner)

        def far_copy(target):
            return remote(mine.at[target], recv.at[q], far_send.at[target], far_recv.at[q], lay.place(target, c))

        def arrival(source):
            return remote(mine.at[source], recv.at[source], far_send.at[source], far_recv.at[source], lay.place(source, c))

        def relay(k):
            pair_copy(k).wait_recv()
            at = pl.ds(k * qpb, qpb)
            mine[at] = part[c, at] + got[at]
            for i in range(qpb):
                target = k * qpb + i

                @pl.when(target != q)
                def _():
                    far_copy(target).start()

        for k in range(blocks):
            both = dot(yt_ref[...], s_ref[:, k * BLOCK : (k + 1) * BLOCK])
            folded = both[:rank] + both[rank:]
            for i in range(BLOCK // share):
                dq, dc = lay.of_device(k * (BLOCK // share) + i)
                part[dc, dq] = pack(folded[:, i * share : (i + 1) * share], share)
            if k == 0 and part is part1:
                pl.semaphore_wait(barrier, n - 1)
            pair_copy(k).start()
            if k >= LAG:
                relay(k - LAG)
        for k in range(blocks - LAG, blocks):
            relay(k)

        def collect():
            def one(i, total):
                source = (q + i) % m
                arrival(source).wait_recv()
                return total + recv[source]

            return lax.fori_loop(1, m, one, mine[q])

        def drain():
            for k in range(blocks):
                pair_copy(k).wait_send()
            each_other(lambda target: far_copy(target).wait_send())

        return collect, drain

    cat_ref[...] = jnp.concatenate(split(start_ref[...].T), axis=1)
    for b in range(load):
        fetch(b).wait()
        forward(b)
    collect1, drain1 = scatter(part1, got1, mine1, recv1, pair_send1, pair_recv1, far_send1, far_recv1)
    full_ref[c, q] = collect1()

    def spread(target):
        return remote(full_ref.at[c, q], full_ref.at[c, q], all_send.at[target], all_recv.at[q], lay.place(target, c))

    def landed(source):
        return remote(
            full_ref.at[c, source], full_ref.at[c, source], all_send.at[source], all_recv.at[source], lay.place(source, c)
        )

    def across(source, half):
        return remote(
            full_ref.at[half, source], full_ref.at[half, source], fwd_send.at[source], fwd_recv.at[source], partner
        )

    each_other(lambda target: spread(target).start())
    across(q, c).start()

    def pass_on(source):
        landed(source).wait_recv()
        across(source, c).start()

    each_other(pass_on)
    across(q, 1 - c).wait_recv()
    each_other(lambda source: across(source, 1 - c).wait_recv())

    per = LANES // share
    for b in range(width // LANES):
        pieces = []
        for i in range(per):
            dq, dc = lay.of_device(b * per + i)
            pieces.append(unpack(full_ref[dc, dq], share))
        pt_ref[:, b * LANES : (b + 1) * LANES] = jnp.concatenate(pieces, axis=1) if per > 1 else pieces[0]
    cat_ref[...] = jnp.concatenate(split(pt_ref[...].T), axis=1)
    for b in range(load):
        forward(b)
    collect2, drain2 = scatter(part2, got2, mine2, recv2, pair_send2, pair_recv2, far_send2, far_recv2)

    phigh, plow = split(pt_ref[...])
    corr = dot(phigh, phigh, NT) + (dot(phigh, plow, NT) + dot(plow, phigh, NT))
    inverse = invert_factor(corr, work_ref)
    icat = jnp.concatenate(split(inverse), axis=0)
    ihigh = icat[:rank]
    for b in range(load):
        at = slice(b * chunk, (b + 1) * chunk)
        both = dot(icat, yt_ref[:rank, at])
        modes = both[:rank] + (both[rank:] + dot(ihigh, yt_ref[rank:, at]))
        proj_ref[:, at] = modes.astype(BF16)
    quad_copy.wait()
    qhigh, qlow = split(quad_vmem[...])
    qcat_ref[:rank, :] = qhigh
    qcat_ref[rank:, :] = qlow

    z = jnp.dot(inverse, unpack(collect2(), share), precision=HIGHEST, preferred_element_type=F32) * scale
    reduced = z.T
    red_ref[...] = reduced
    edge_ref[...] = reduced[:SUBLANES]
    before = (me + n - 1) % n
    edge = remote(edge_ref, halo_ref, edge_send, edge_recv, (before // lay.slab, before % lay.slab))
    edge.start()

    lin_t, off_t = lin_ref[...].T, off_ref[...].T
    state = z
    for _ in range(2):
        pairs = (state[:, None, :] * state[None, :, :]).reshape(rank * rank, share)
        pair_high, pair_low = split(pairs)
        both = dot(qcat_ref[...], pair_high)
        quad = both[:rank] + (both[rank:] + dot(qcat_ref[:rank, :], pair_low))
        change = jnp.dot(lin_t, state, precision=HIGHEST, preferred_element_type=F32) + quad + off_t
        state = state + 0.25 * change
    edge.wait_recv()
    target = jnp.concatenate([z[:, 2:], halo_ref[...].T[:, :2]], axis=1)
    position = me * share + lax.broadcasted_iota(jnp.int32, (1, share), 1)
    mis_ref[...] = jnp.where(position < width - 2, state - target, 0.0).T

    edge.wait_send()
    drain1()
    drain2()
    each_other(lambda other: spread(other).wait_send())
    across(q, c).wait_send()
    each_other(lambda other: across(other, c).wait_send())


def emit_kernel(proj_in, red_in, mis_in, proj_ref, red_ref, mis_ref):
    proj_ref[...] = proj_in[...]
    red_ref[...] = red_in[...]
    mis_ref[...] = mis_in[...]


def invert_factor(corr, work_ref):
    rank = corr.shape[0]
    row = lax.broadcasted_iota(jnp.int32, (rank, rank), 0)
    col = lax.broadcasted_iota(jnp.int32, (rank, rank), 1)
    eye = jnp.where(row == col, 1.0, 0.0).astype(F32)
    work_ref[...] = jnp.concatenate([corr, eye], axis=1)
    rows1 = lax.broadcasted_iota(jnp.int32, (rank, 1), 0)
    lanes = lax.broadcasted_iota(jnp.int32, (rank, 2 * rank), 1)
    lane1 = lax.broadcasted_iota(jnp.int32, (1, 2 * rank), 1)

    def eliminate(j, _):
        m = work_ref[...]
        pivot = work_ref[pl.ds(j, 1), :]
        column = jnp.sum(jnp.where(lanes == j, m, 0.0), axis=1, keepdims=True)
        d = jnp.sum(jnp.where(lane1 == j, pivot, 0.0), axis=1, keepdims=True)
        factor = jnp.where(rows1 > j, column / d, 0.0)
        work_ref[...] = m - factor * pivot
        return 0

    lax.fori_loop(0, rank, eliminate, 0)
    m = work_ref[...]
    diag = jnp.sum(jnp.where(row == col, m[:, :rank], 0.0), axis=1, keepdims=True)
    return m[:, rank:] / jnp.sqrt(diag)


def body(snapshots, start_block, linear_op, quad_op, offset, *, lay):
    rows, width = snapshots.shape
    rank = start_block.shape[1]
    n, m = lay.n, lay.m
    share = width // n
    tall = rank * share // LANES
    blocks = width // BLOCK
    load = 4
    scale = math.sqrt(width) / (rows * n)
    dma = lambda k: pltpu.SemaphoreType.DMA((k,))
    half = lambda: pltpu.VMEM((m, tall, LANES), F32)
    both = lambda: pltpu.VMEM((2, m, tall, LANES), F32)
    one = pltpu.SemaphoreType.DMA
    projection, reduced, mismatch = pl.pallas_call(
        functools.partial(kernel, lay, scale),
        in_specs=[ANY_SPEC, VMEM_SPEC, VMEM_SPEC, ANY_SPEC, VMEM_SPEC],
        out_specs=[VMEM_SPEC] * 3,
        out_shape=[
            jax.ShapeDtypeStruct((rank, rows), BF16),
            jax.ShapeDtypeStruct((share, rank), F32),
            jax.ShapeDtypeStruct((share, rank), F32),
        ],
        scratch_shapes=[
            pltpu.VMEM((rows, width), BF16),
            pltpu.VMEM((width, 2 * rank), BF16),
            pltpu.VMEM((2 * rank, rows), BF16),
            pltpu.VMEM((rank, width), F32),
            pltpu.VMEM((rank, rank * rank), F32),
            pltpu.VMEM((2 * rank, rank * rank), BF16),
            pltpu.VMEM((rank, 2 * rank), F32),
            pltpu.VMEM((SUBLANES, rank), F32),
            pltpu.VMEM((SUBLANES, rank), F32),
            both(),
            both(), half(), half(), half(),
            both(), half(), half(), half(),
            dma(load), one,
            dma(blocks), dma(blocks), dma(m), dma(m),
            dma(blocks), dma(blocks), dma(m), dma(m),
            dma(m), dma(m), dma(m), dma(m), one, one,
        ],
        compiler_params=pltpu.CompilerParams(collective_id=0, has_side_effects=True, vmem_limit_bytes=58 * 2**20),
        name="inference",
    )(snapshots, start_block.T, linear_op, quad_op.T, offset.reshape(1, rank))
    projection, reduced, mismatch = pl.pallas_call(
        emit_kernel,
        in_specs=[VMEM_SPEC] * 3,
        out_specs=[VMEM_SPEC] * 3,
        out_shape=[jax.ShapeDtypeStruct(x.shape, x.dtype) for x in (projection, reduced, mismatch)],
        name="emit",
    )(projection, reduced, mismatch)
    return projection.T, reduced, mismatch


def solution(mesh):
    in_specs = (P(("rows", "slab"), None), P(), P(), P(), P())
    out_specs = (P(("rows", "slab"), None), P(("rows", "slab"), None), P(("rows", "slab"), None))
    grid = mesh.devices
    chip = lambda device: getattr(device, "coords", None)
    rows, slab = mesh.shape["rows"], mesh.shape["slab"]
    paired_rows = rows > 1 and chip(grid[0, 0]) is not None and chip(grid[0, 0]) == chip(grid[1, 0])
    lay = Layout(rows, slab, "rows" if paired_rows or slab % 2 else "slab")
    run = functools.partial(body, lay=lay)
    return jax.shard_map(run, mesh=mesh, in_specs=in_specs, out_specs=out_specs, check_vma=False)
```
